32 devices in a mesh: dp: 1 (over z), tp: 32 (over y, x, core).
Axes of the slice: x: 4, y: 4, z: 1, core: 2. Of those that a mesh axis runs over, the one named last changes fastest.
The devices are a block of a 4x4x8 slice.
Arguments:
- act_in: bfloat16 [32, 128, 4096], P('dp')
- ln_gain: float32 [2, 4096], replicated
- ln_bias: float32 [2, 4096], replicated
- w_qkv: bfloat16 [2, 4096, 32, 384], P(None, None, 'tp')
- w_out: bfloat16 [2, 4096, 4096], P(None, 'tp')
- w_up: bfloat16 [2, 4096, 16384], P(None, None, 'tp')
- w_down: bfloat16 [2, 16384, 4096], P(None, 'tp')
Outputs:
- output: bfloat16 [32, 128, 4096], P('dp')
All inputs are finite; a program needn't handle non-finite values.
Results may differ from the reference program's by a relative error of at most 0.02.
Values are sent between devices in bfloat16 or wider.
A program may use at most 768 MiB of HBM per device.

```python
import math
import jax
import jax.numpy as jnp
from jax import lax

D_MODEL = 4096
HEADS = 32
KV_HEADS = 32
HEAD_DIM = 128
FF_DIM = 16384
BATCH = 32
SEQ_LEN = 128
LAYERS = 2

GROUP_HEADS = HEADS // KV_HEADS
LN_EPS = 1e-5
ROPE_BASE = 10000.0
QUERY_GAIN = 2.0


def setup_inputs(seed: int = 0, part: int = 0) -> dict:
    base_key = jax.random.key(seed)
    part_key = jax.random.fold_in(base_key, part)
    key_list = jax.random.split(base_key, 6)
    group_cols = (GROUP_HEADS + 2) * HEAD_DIM
    col_gain = jnp.where(jnp.arange(group_cols) < GROUP_HEADS * HEAD_DIM, QUERY_GAIN, 1.0)
    act_in = jax.random.normal(part_key, (BATCH, SEQ_LEN, D_MODEL), jnp.float32)
    ln_gain = 1.0 + 0.2 * jax.random.normal(key_list[0], (LAYERS, D_MODEL), jnp.float32)
    ln_bias = 0.3 * jax.random.normal(key_list[1], (LAYERS, D_MODEL), jnp.float32)
    w_qkv = jax.random.normal(key_list[2], (LAYERS, D_MODEL, KV_HEADS, group_cols), jnp.float32) * col_gain * D_MODEL ** -0.5
    w_out = jax.random.normal(key_list[3], (LAYERS, HEADS * HEAD_DIM, D_MODEL), jnp.float32) * (1.5 * (HEADS * HEAD_DIM) ** -0.5)
    w_up = jax.random.normal(key_list[4], (LAYERS, D_MODEL, FF_DIM), jnp.float32) * D_MODEL ** -0.5
    w_down = jax.random.normal(key_list[5], (LAYERS, FF_DIM, D_MODEL), jnp.float32) * FF_DIM ** -0.5
    return {"act_in": act_in.astype(jnp.bfloat16), "ln_gain": ln_gain, "ln_bias": ln_bias, "w_qkv": w_qkv.astype(jnp.bfloat16), "w_out": w_out.astype(jnp.bfloat16), "w_up": w_up.astype(jnp.bfloat16), "w_down": w_down.astype(jnp.bfloat16)}


def layer_norm(hidden, gain, bias):
    hidden_f = hidden.astype(jnp.float32)
    row_mean = jnp.mean(hidden_f, axis=-1, keepdims=True)
    centered = hidden_f - row_mean
    row_var = jnp.mean(centered * centered, axis=-1, keepdims=True)
    return (centered * lax.rsqrt(row_var + LN_EPS) * gain + bias).astype(jnp.bfloat16)


def rope_tables():
    half_dim = HEAD_DIM // 2
    inv_freq = ROPE_BASE ** (-2.0 * jnp.arange(half_dim, dtype=jnp.float32) / HEAD_DIM)
    angles = jnp.arange(SEQ_LEN, dtype=jnp.float32)[:, None] * inv_freq[None, :]
    return jnp.cos(angles), jnp.sin(angles)


def apply_rope(proj, cos_tab, sin_tab):
    half_dim = proj.shape[-1] // 2
    first = proj[..., :half_dim]
    second = proj[..., half_dim:]
    return jnp.concatenate([first * cos_tab - second * sin_tab, second * cos_tab + first * sin_tab], axis=-1)


def attend_sequence(operands):
    query, keys, values = operands
    scores = jnp.einsum("sgrd,tgd->grst", query.astype(jnp.float32), keys.astype(jnp.float32)) / math.sqrt(HEAD_DIM)
    positions = jnp.arange(SEQ_LEN)
    allowed = positions[:, None] >= positions[None, :]
    scores = jnp.where(allowed, scores, -1e30)
    attn_probs = jax.nn.softmax(scores, axis=-1).astype(jnp.bfloat16)
    context = jnp.einsum("grst,tgd->sgrd", attn_probs.astype(jnp.float32), values.astype(jnp.float32))
    return context.astype(jnp.bfloat16)


def layer_step(hidden, params):
    gain, bias, w_qkv, w_out, w_up, w_down = params
    normed = layer_norm(hidden, gain, bias)
    flat = normed.reshape(BATCH * SEQ_LEN, D_MODEL)
    qkv_proj = jnp.dot(flat, w_qkv.reshape(D_MODEL, -1), preferred_element_type=jnp.float32)
    qkv_proj = qkv_proj.reshape(BATCH, SEQ_LEN, KV_HEADS, GROUP_HEADS + 2, HEAD_DIM)
    cos_tab, sin_tab = rope_tables()
    query = apply_rope(qkv_proj[:, :, :, :GROUP_HEADS], cos_tab[None, :, None, None, :], sin_tab[None, :, None, None, :]).astype(jnp.bfloat16)
    keys = apply_rope(qkv_proj[:, :, :, GROUP_HEADS], cos_tab[None, :, None, :], sin_tab[None, :, None, :]).astype(jnp.bfloat16)
    values = qkv_proj[:, :, :, GROUP_HEADS + 1].astype(jnp.bfloat16)
    context = lax.map(attend_sequence, (query, keys, values))
    attn_part = jnp.dot(context.reshape(BATCH * SEQ_LEN, HEADS * HEAD_DIM), w_out, preferred_element_type=jnp.float32)
    up_proj = jnp.dot(flat, w_up, preferred_element_type=jnp.float32)
    gelu_out = jax.nn.gelu(up_proj, approximate=False).astype(jnp.bfloat16)
    mlp_part = jnp.dot(gelu_out, w_down, preferred_element_type=jnp.float32)
    update = (attn_part + mlp_part).astype(jnp.bfloat16).reshape(BATCH, SEQ_LEN, D_MODEL)
    new_hidden = (hidden.astype(jnp.float32) + update.astype(jnp.float32)).astype(jnp.bfloat16)
    return new_hidden, None


def reference(act_in, ln_gain, ln_bias, w_qkv, w_out, w_up, w_down):
    act_out = lax.scan(layer_step, act_in, (ln_gain, ln_bias, w_qkv, w_out, w_up, w_down))[0]
    return act_out
```

```python
import functools
import math

import jax
import jax.numpy as jnp
from jax import lax
from jax.experimental import pallas as pl
from jax.experimental.pallas import tpu as pltpu
from jax.sharding import PartitionSpec as P

LN_EPS = 1e-5
ROPE_BASE = 10000.0
CORES = 2
RINGS = 4
MESH_ID = pl.DeviceIdType.MESH
BF16 = jnp.bfloat16
F32 = jnp.float32
VMEM_LIMIT = 66_000_000


def layer_norm(hidden, gain, bias):
    hidden_f = hidden.astype(F32)
    row_mean = jnp.mean(hidden_f, axis=-1, keepdims=True)
    centered = hidden_f - row_mean
    row_var = jnp.mean(centered * centered, axis=-1, keepdims=True)
    return (centered * lax.rsqrt(row_var + LN_EPS) * gain + bias).astype(BF16)


def rope_tables(seq_len, head_dim):
    half_dim = head_dim // 2
    inv_freq = ROPE_BASE ** (-2.0 * jnp.arange(half_dim, dtype=F32) / head_dim)
    angles = jnp.arange(seq_len, dtype=F32)[:, None] * inv_freq[None, :]
    return jnp.cos(angles), jnp.sin(angles)


def apply_rope(proj, cos_tab, sin_tab):
    half_dim = proj.shape[-1] // 2
    first = proj[..., :half_dim]
    second = proj[..., half_dim:]
    return jnp.concatenate([first * cos_tab - second * sin_tab, second * cos_tab + first * sin_tab], axis=-1)


def attend(qkv, head_dim):
    seq_len = qkv.shape[1]
    cos_tab, sin_tab = rope_tables(seq_len, head_dim)
    query = apply_rope(qkv[..., :head_dim], cos_tab, sin_tab).astype(BF16)
    keys = apply_rope(qkv[..., head_dim:2 * head_dim], cos_tab, sin_tab).astype(BF16)
    values = qkv[..., 2 * head_dim:].astype(BF16)
    scores = jnp.einsum("bsd,btd->bst", query, keys, preferred_element_type=F32) * (head_dim ** -0.5)
    positions = jnp.arange(seq_len)
    scores = jnp.where(positions[:, None] >= positions[None, :], scores, -1e30)
    probs = jax.nn.softmax(scores, axis=-1).astype(BF16)
    return jnp.einsum("bst,btd->bsd", probs, values, preferred_element_type=F32).astype(BF16)


class Torus:
    def __init__(self, side):
        self.side = side
        self.chips = side * side

    def me(self):
        idx = lax.axis_index("tp")
        core = lax.rem(idx, CORES)
        chip = lax.div(idx, CORES)
        return core, lax.rem(chip, self.side), lax.div(chip, self.side)

    def position(self, ring, x, y):
        major = y if ring < 2 else x
        return self.side * major + lax.rem(x + y, self.side)

    def chip_at(self, ring, pos):
        pos = lax.rem(pos + 2 * self.chips, self.chips)
        major = lax.div(pos, self.side)
        minor = lax.rem(lax.rem(pos, self.side) - major + self.side, self.side)
        return major * self.side + minor if ring < 2 else minor * self.side + major

    def sign(self, ring):
        return 1 if ring % 2 == 0 else -1


def enter(torus, core, pos, extra=()):
    barrier = pltpu.get_barrier_semaphore()
    nexts = []
    for ring in range(RINGS):
        chip = torus.chip_at(ring, pos[ring] + torus.sign(ring))
        nexts.append(chip * CORES + core)
    for device in [*nexts, *extra]:
        pl.semaphore_signal(barrier, inc=1, device_id={"tp": device}, device_id_type=MESH_ID)
    pl.semaphore_wait(barrier, RINGS + len(extra))
    return nexts


def reduce_kernel(torus, ctx0, ctx1, up0, up1, wo0, wo1, wd0, wd1, res_ref, gain_ref, bias_ref, x_ref, n_ref,
                  h_buf, w_buf, part, acc, load_sem, send_sem, recv_sem):
    core, x, y = torus.me()
    pos = [torus.position(ring, x, y) for ring in range(RINGS)]
    heads, cols = ctx0.shape[2], up0.shape[2]
    d_model = w_buf.shape[1]
    quarter = d_model // RINGS
    rows = h_buf.shape[1]
    last = torus.chips - 1

    copies = []
    start = 0
    for i, (h_src, w_src, width) in enumerate(((ctx0, wo0, heads), (up0, wd0, cols), (ctx1, wo1, heads), (up1, wd1, cols))):
        copies.append(pltpu.make_async_copy(h_src, h_buf.at[:, :, pl.ds(start, width)], load_sem.at[2 * i]))
        copies.append(pltpu.make_async_copy(w_src, w_buf.at[pl.ds(start, width), :], load_sem.at[2 * i + 1]))
        start += width
    for copy in copies:
        copy.start()
    nexts = enter(torus, core, pos)
    for copy in copies:
        copy.wait()

    tile = min(512, quarter)

    def compute(step):
        for ring in range(RINGS):
            block = torus.chip_at(ring, pos[ring] - torus.sign(ring) * (1 + step))

            @pl.loop(0, quarter // tile)
            def _(j):
                off = pl.multiple_of(j * tile, tile)
                part[ring, :, pl.ds(off, tile)] = jnp.dot(
                    h_buf[block], w_buf[:, pl.ds(pl.multiple_of(ring * quarter + off, tile), tile)],
                    preferred_element_type=F32)

    def send(ring, step):
        return pltpu.make_async_remote_copy(
            src_ref=acc.at[ring, step], dst_ref=acc.at[ring, step + 1], send_sem=send_sem.at[ring],
            recv_sem=recv_sem.at[ring, step], device_id={"tp": nexts[ring]}, device_id_type=MESH_ID)

    compute(0)
    for ring in range(RINGS):
        acc[ring, 0] = part[ring].astype(BF16)
        send(ring, 0).start()

    @pl.loop(1, last)
    def _(step):
        compute(step)
        for ring in range(RINGS):
            send(ring, step - 1).wait_recv()
            acc[ring, step] = (acc[ring, step].astype(F32) + part[ring]).astype(BF16)
            send(ring, step).start()

    compute(last)
    for ring in range(RINGS):
        send(ring, last - 1).wait_recv()

    chunk = 16

    @pl.loop(0, rows // chunk)
    def _(i):
        rs = pl.ds(pl.multiple_of(i * chunk, chunk), chunk)
        total = jnp.concatenate([acc[ring, last, rs].astype(F32) + part[ring, rs] for ring in range(RINGS)], axis=1)
        new = (res_ref[rs].astype(F32) + total.astype(BF16).astype(F32)).astype(BF16)
        x_ref[rs] = new
        n_ref[rs] = layer_norm(new, gain_ref[...], bias_ref[...])

    for ring in range(RINGS):
        done = acc.at[ring, pl.ds(0, last)]
        pltpu.make_async_copy(done, done, send_sem.at[ring]).wait()


def reduce_layer(torus, ctxs, ups, w_outs, w_downs, residual, gain, bias):
    rows, d_model = residual.shape
    depth = sum(a.shape[2] for a in (*ctxs, *ups))
    quarter = d_model // RINGS
    anys = [pl.BlockSpec(memory_space=pl.ANY)] * 8
    vmem = pl.BlockSpec(memory_space=pltpu.VMEM)
    return pl.pallas_call(
        functools.partial(reduce_kernel, torus),
        name="reduce_layer",
        out_shape=[jax.ShapeDtypeStruct((rows, d_model), BF16)] * 2,
        in_specs=[*anys, vmem, vmem, vmem],
        out_specs=[vmem, vmem],
        scratch_shapes=[
            pltpu.VMEM((torus.chips, rows, depth), BF16),
            pltpu.VMEM((depth, d_model), BF16),
            pltpu.VMEM((RINGS, rows, quarter), F32),
            pltpu.VMEM((RINGS, torus.chips, rows, quarter), BF16),
            pltpu.SemaphoreType.DMA((8,)),
            pltpu.SemaphoreType.DMA((RINGS,)),
            pltpu.SemaphoreType.DMA((RINGS, torus.chips - 1)),
        ],
        compiler_params=pltpu.CompilerParams(collective_id=0, has_side_effects=True, vmem_limit_bytes=VMEM_LIMIT),
    )(*ctxs, *ups, *w_outs, *w_downs, residual, gain.reshape(1, -1), bias.reshape(1, -1))


def project_kernel(torus, n_ref, wq0, wu0, wq1, wu1, out_ref, w_buf, got, stage, load_sem, send_sem, recv_sem):
    core, x, y = torus.me()
    pos = [torus.position(ring, x, y) for ring in range(RINGS)]
    rows = n_ref.shape[0]
    share = rows // RINGS
    last = torus.chips - 1
    copies = []
    start = 0
    for i, w_src in enumerate((wq0, wu0, wq1, wu1)):
        width = w_src.shape[1]
        copies.append(pltpu.make_async_copy(w_src, w_buf.at[:, pl.ds(start, width)], load_sem.at[i]))
        start += width
    own_chip = y * torus.side + x
    own = pltpu.make_async_copy(n_ref, got.at[own_chip], load_sem.at[4])
    own.start()
    for copy in copies:
        copy.start()
    nexts = enter(torus, core, pos)
    own.wait()

    def block(ring, step):
        return torus.chip_at(ring, pos[ring] - torus.sign(ring) * step)

    def piece(ring, step):
        return got.at[block(ring, step), pl.ds(ring * share, share)]

    def send(ring, step):
        return pltpu.make_async_remote_copy(
            src_ref=piece(ring, step), dst_ref=piece(ring, step), send_sem=send_sem.at[ring],
            recv_sem=recv_sem.at[ring, step], device_id={"tp": nexts[ring]}, device_id_type=MESH_ID)

    def arrived(ring, step):
        return pltpu.make_async_remote_copy(
            src_ref=piece(ring, step + 1), dst_ref=piece(ring, step + 1), send_sem=send_sem.at[ring],
            recv_sem=recv_sem.at[ring, step], device_id={"tp": nexts[ring]}, device_id_type=MESH_ID)

    width = w_buf.shape[1]
    tile = 256

    def compute(step):
        for ring in range(RINGS):
            stage[pl.ds(ring * share, share)] = got[block(ring, step), pl.ds(ring * share, share)]

        @pl.loop(0, width // tile)
        def _(j):
            cs = pl.ds(pl.multiple_of(j * tile, tile), tile)
            res = jnp.dot(stage[...], w_buf[:, cs], preferred_element_type=F32)
            for ring in range(RINGS):
                rs = slice(ring * share, (ring + 1) * share)
                out_ref[block(ring, step), rs, cs] = res[rs]

    for ring in range(RINGS):
        send(ring, 0).start()
    for copy in copies:
        copy.wait()
    compute(0)

    @pl.loop(1, last)
    def _(step):
        for ring in range(RINGS):
            arrived(ring, step - 1).wait_recv()
            send(ring, step).start()
        compute(step)

    for ring in range(RINGS):
        arrived(ring, last - 1).wait_recv()
    compute(last)
    for ring in range(RINGS):
        done = got.at[pl.ds(0, last), pl.ds(ring * share, share)]
        pltpu.make_async_copy(done, done, send_sem.at[ring]).wait()


def gather_project(torus, normed, w_qkvs, w_ups):
    rows, d_model = normed.shape
    width = sum(w.shape[1] for w in (*w_qkvs, *w_ups))
    anys = [pl.BlockSpec(memory_space=pl.ANY)] * 5
    return pl.pallas_call(
        functools.partial(project_kernel, torus),
        name="gather_project",
        out_shape=jax.ShapeDtypeStruct((torus.chips, rows, width), F32),
        in_specs=anys,
        out_specs=pl.BlockSpec(memory_space=pltpu.VMEM),
        scratch_shapes=[
            pltpu.VMEM((d_model, width), BF16),
            pltpu.VMEM((torus.chips, rows, d_model), BF16),
            pltpu.VMEM((rows, d_model), BF16),
            pltpu.SemaphoreType.DMA((5,)),
            pltpu.SemaphoreType.DMA((RINGS,)),
            pltpu.SemaphoreType.DMA((RINGS, torus.chips - 1)),
        ],
        compiler_params=pltpu.CompilerParams(collective_id=1, has_side_effects=True, vmem_limit_bytes=VMEM_LIMIT),
    )(normed, w_qkvs[0], w_ups[0], w_qkvs[1], w_ups[1])


def gather_kernel(torus, y_ref, out_ref, got, load_sem, send_sem, recv_sem, pair_sem, store_sem):
    core, x, y = torus.me()
    pos = [torus.position(ring, x, y) for ring in range(RINGS)]
    rows = y_ref.shape[0]
    share = rows // RINGS
    last = torus.chips - 1
    own_chip = y * torus.side + x
    own = pltpu.make_async_copy(y_ref, got.at[own_chip], load_sem.at[0])
    own.start()
    partner = own_chip * CORES + (CORES - 1 - core)
    nexts = enter(torus, core, pos, (partner,))
    own.wait()

    def block(ring, step):
        return torus.chip_at(ring, pos[ring] - torus.sign(ring) * step)

    def piece(ring, step):
        return got.at[block(ring, step), pl.ds(ring * share, share)]

    def send(ring, step):
        return pltpu.make_async_remote_copy(
            src_ref=piece(ring, step), dst_ref=piece(ring, step), send_sem=send_sem.at[ring],
            recv_sem=recv_sem.at[ring, step], device_id={"tp": nexts[ring]}, device_id_type=MESH_ID)

    def arrived(ring, step):
        return pltpu.make_async_remote_copy(
            src_ref=piece(ring, step + 1), dst_ref=piece(ring, step + 1), send_sem=send_sem.at[ring],
            recv_sem=recv_sem.at[ring, step], device_id={"tp": nexts[ring]}, device_id_type=MESH_ID)

    def spread(ring, step):
        dst = out_ref.at[core * torus.chips + block(ring, step), pl.ds(ring * share, share)]
        pltpu.make_async_remote_copy(
            src_ref=piece(ring, step), dst_ref=dst, send_sem=pair_sem.at[0], recv_sem=pair_sem.at[1],
            device_id={"tp": partner}, device_id_type=MESH_ID).start()
        pltpu.make_async_copy(piece(ring, step), dst, store_sem.at[0]).start()

    for ring in range(RINGS):
        send(ring, 0).start()
    for ring in range(RINGS):
        spread(ring, 0)

    @pl.loop(1, last)
    def _(step):
        for ring in range(RINGS):
            arrived(ring, step - 1).wait_recv()
            send(ring, step).start()
        for ring in range(RINGS):
            spread(ring, step)

    for ring in range(RINGS):
        arrived(ring, last - 1).wait_recv()
        spread(ring, last)
    for ring in range(RINGS):
        done = got.at[pl.ds(0, last), pl.ds(ring * share, share)]
        pltpu.make_async_copy(done, done, send_sem.at[ring]).wait()
    pltpu.make_async_copy(got, got, pair_sem.at[0]).wait()
    pltpu.make_async_copy(got, got, store_sem.at[0]).wait()
    pltpu.make_async_copy(got, got, pair_sem.at[1]).wait()


def gather_all(torus, y_own):
    rows, d_model = y_own.shape
    return pl.pallas_call(
        functools.partial(gather_kernel, torus),
        name="gather_all",
        out_shape=jax.ShapeDtypeStruct((CORES * torus.chips, rows, d_model), BF16),
        in_specs=[pl.BlockSpec(memory_space=pl.ANY)],
        out_specs=pl.BlockSpec(memory_space=pl.ANY),
        scratch_shapes=[
            pltpu.VMEM((torus.chips, rows, d_model), BF16),
            pltpu.SemaphoreType.DMA((1,)),
            pltpu.SemaphoreType.DMA((RINGS,)),
            pltpu.SemaphoreType.DMA((RINGS, torus.chips - 1)),
            pltpu.SemaphoreType.DMA((2,)),
            pltpu.SemaphoreType.DMA((1,)),
        ],
        compiler_params=pltpu.CompilerParams(collective_id=2, has_side_effects=True, vmem_limit_bytes=VMEM_LIMIT),
    )(y_own)


def solution(mesh):
    n_tp = mesh.shape["tp"]
    torus = Torus(math.isqrt(n_tp // CORES))
    swap = [(i, i ^ 1) for i in range(n_tp)]

    def shard_body(act_in, ln_gain, ln_bias, w_qkv, w_out, w_up, w_down):
        layers = ln_gain.shape[0]
        head_dim = w_out.shape[1]
        idx = lax.axis_index("tp")
        core, chip = lax.rem(idx, CORES), lax.div(idx, CORES)
        w_qkv = w_qkv[:, :, 0]
        mine = [[w[layer] for layer in range(layers)] for w in (w_qkv, w_up, w_out, w_down)]
        theirs = [[lax.ppermute(w[layer], "tp", swap) for layer in range(layers)] for w in mine]
        w_qkvs, w_ups, w_outs, w_downs = [list(zip(a, b)) for a, b in zip(mine, theirs)]

        half = lax.dynamic_slice_in_dim(act_in, core * torus.chips, torus.chips, 0)
        own = lax.dynamic_index_in_dim(half, chip, 0, keepdims=False)
        normed = layer_norm(half, ln_gain[0], ln_bias[0])
        for layer in range(layers):
            if layer == 0:
                qkvs = [jnp.einsum("bsd,dc->bsc", normed, w, preferred_element_type=F32) for w in w_qkvs[0]]
                raws = [jnp.einsum("bsd,dc->bsc", normed, w, preferred_element_type=F32) for w in w_ups[0]]
            else:
                proj = gather_project(torus, normed, w_qkvs[layer], w_ups[layer])
                nq, nu = w_qkvs[layer][0].shape[1], w_ups[layer][0].shape[1]
                qkvs = [proj[..., i * (nq + nu):i * (nq + nu) + nq] for i in range(CORES)]
                raws = [proj[..., i * (nq + nu) + nq:(i + 1) * (nq + nu)] for i in range(CORES)]
            ctxs = [attend(qkv, head_dim) for qkv in qkvs]
            ups = [jax.nn.gelu(raw, approximate=False).astype(BF16) for raw in raws]
            nxt = (layer + 1) % layers
            own, normed = reduce_layer(torus, ctxs, ups, w_outs[layer], w_downs[layer], own, ln_gain[nxt], ln_bias[nxt])
        return gather_all(torus, own)

    return jax.shard_map(shard_body, mesh=mesh, in_specs=(P("dp", None, None), P(None, None), P(None, None), P(None, None, "tp", None), P(None, "tp", None), P(None, None, "tp"), P(None, "tp", None)), out_specs=P("dp", None, None), check_vma=False)
```

```python
import functools
import math

import jax
import jax.numpy as jnp
from jax import lax
from jax.experimental import pallas as pl
from jax.experimental.pallas import tpu as pltpu
from jax.sharding import PartitionSpec as P

LN_EPS = 1e-5
ROPE_BASE = 10000.0
CORES = 2
RINGS = 4
SUBS = 2
MESH_ID = pl.DeviceIdType.MESH
BF16 = jnp.bfloat16
F32 = jnp.float32
VMEM_LIMIT = 66_000_000


def layer_norm(hidden, gain, bias):
    hidden_f = hidden.astype(F32)
    row_mean = jnp.mean(hidden_f, axis=-1, keepdims=True)
    centered = hidden_f - row_mean
    row_var = jnp.mean(centered * centered, axis=-1, keepdims=True)
    return (centered * lax.rsqrt(row_var + LN_EPS) * gain + bias).astype(BF16)


def rope_tables(seq_len, head_dim):
    half_dim = head_dim // 2
    inv_freq = ROPE_BASE ** (-2.0 * jnp.arange(half_dim, dtype=F32) / head_dim)
    angles = jnp.arange(seq_len, dtype=F32)[:, None] * inv_freq[None, :]
    return jnp.cos(angles), jnp.sin(angles)


def apply_rope(proj, cos_tab, sin_tab):
    half_dim = proj.shape[-1] // 2
    first = proj[..., :half_dim]
    second = proj[..., half_dim:]
    return jnp.concatenate([first * cos_tab - second * sin_tab, second * cos_tab + first * sin_tab], axis=-1)


def attend(qkv, head_dim):
    seq_len = qkv.shape[1]
    cos_tab, sin_tab = rope_tables(seq_len, head_dim)
    query = apply_rope(qkv[..., :head_dim], cos_tab, sin_tab).astype(BF16)
    keys = apply_rope(qkv[..., head_dim:2 * head_dim], cos_tab, sin_tab).astype(BF16)
    values = qkv[..., 2 * head_dim:].astype(BF16)
    scores = jnp.einsum("bsd,btd->bst", query, keys, preferred_element_type=F32) * (head_dim ** -0.5)
    positions = jnp.arange(seq_len)
    scores = jnp.where(positions[:, None] >= positions[None, :], scores, -1e30)
    probs = jax.nn.softmax(scores, axis=-1).astype(BF16)
    return jnp.einsum("bst,btd->bsd", probs, values, preferred_element_type=F32).astype(BF16)


class Torus:
    def __init__(self, side):
        self.side = side
        self.chips = side * side

    def me(self):
        idx = lax.axis_index("tp")
        core = lax.rem(idx, CORES)
        chip = lax.div(idx, CORES)
        return core, lax.rem(chip, self.side), lax.div(chip, self.side)

    def position(self, ring, x, y):
        major = y if ring < 2 else x
        return self.side * major + lax.rem(x + y, self.side)

    def chip_at(self, ring, pos):
        pos = lax.rem(pos + 2 * self.chips, self.chips)
        major = lax.div(pos, self.side)
        minor = lax.rem(lax.rem(pos, self.side) - major + self.side, self.side)
        return major * self.side + minor if ring < 2 else minor * self.side + major

    def sign(self, ring):
        return 1 if ring % 2 == 0 else -1


def enter(torus, core, pos, extra=()):
    barrier = pltpu.get_barrier_semaphore()
    nexts = []
    for ring in range(RINGS):
        chip = torus.chip_at(ring, pos[ring] + torus.sign(ring))
        nexts.append(chip * CORES + core)
    for device in [*nexts, *extra]:
        pl.semaphore_signal(barrier, inc=1, device_id={"tp": device}, device_id_type=MESH_ID)
    pl.semaphore_wait(barrier, RINGS + len(extra))
    return nexts


def gelu(x):
    return 0.5 * x * (1.0 + lax.erf(x * (0.5 ** 0.5)))


def reduce_kernel(torus, layer, from_normed, last_layer, *refs):
    (src_ref, ctx0, ctx1, wo0, wo1, wd0, wd1, wu0, wu1, res_ref, gain_ref, bias_ref), refs = refs[:12], refs[12:]
    if last_layer:
        x_ref, n_ref, refs = refs[0], None, refs[1:]
    else:
        x_ref, n_ref, refs = refs[0], refs[1], refs[2:]
    ctx_buf, w_buf, up_buf, rows_buf, stage, part, acc, load_sem, row_sem, send_sem, recv_sem = refs
    core, x, y = torus.me()
    pos = [torus.position(ring, x, y) for ring in range(RINGS)]
    heads, cols = ctx0.shape[2], wd0.shape[1]
    d_model = w_buf.shape[1]
    rows = stage.shape[0]
    share = rows // RINGS
    last = torus.chips - 1
    ctx_width = CORES * heads

    def block(ring, step):
        return torus.chip_at(ring, pos[ring] - torus.sign(ring) * (1 + step))

    def fetch(ring, step, slot):
        return pltpu.make_async_copy(
            src_ref.at[block(ring, step), pl.ds(ring * share, share)],
            rows_buf.at[slot, pl.ds(ring * share, share)], row_sem.at[slot, ring])

    for ring in range(RINGS):
        fetch(ring, 0, 0).start()
    copies = []
    if from_normed:
        for i, w_src in enumerate((wu0, wu1)):
            copies.append(pltpu.make_async_copy(w_src.at[layer], up_buf.at[:, pl.ds(i * cols, cols)], load_sem.at[i]))
    for i, src in enumerate((ctx0, ctx1)):
        copies.append(pltpu.make_async_copy(src, ctx_buf.at[:, :, pl.ds(i * heads, heads)], load_sem.at[2 + i]))
    start = 0
    for i, (w_src, width) in enumerate(((wo0, heads), (wo1, heads), (wd0, cols), (wd1, cols))):
        copies.append(pltpu.make_async_copy(w_src.at[layer], w_buf.at[pl.ds(start, width), :], load_sem.at[4 + i]))
        start += width
    for copy in copies:
        copy.start()
    nexts = enter(torus, core, pos)
    for copy in copies:
        copy.wait()

    tile = 256
    wide = 512

    def compute(step, slot, more):
        if more:
            for ring in range(RINGS):
                fetch(ring, step + 1, 1 - slot).start()
        for ring in range(RINGS):
            stage[pl.ds(ring * share, share), 0:ctx_width] = ctx_buf[block(ring, step), pl.ds(ring * share, share)]
            fetch(ring, step, slot).wait()
        if from_normed:
            @pl.loop(0, CORES * cols // tile)
            def _(j):
                cs = pl.multiple_of(j * tile, tile)
                raw = jnp.dot(rows_buf[slot], up_buf[:, pl.ds(cs, tile)], preferred_element_type=F32)
                stage[:, pl.ds(pl.multiple_of(ctx_width + cs, 128), tile)] = gelu(raw).astype(BF16)
        else:
            stage[:, ctx_width:] = rows_buf[slot]

    narrow = d_model // SUBS

    def down(sub):
        @pl.loop(0, narrow // wide)
        def _(j):
            cs = pl.ds(pl.multiple_of(sub * narrow + j * wide, wide), wide)
            part[:, cs] = jnp.dot(stage[...], w_buf[:, cs], preferred_element_type=F32)

    def mine(ring, sub):
        return part[pl.ds(ring * share, share), sub * narrow:(sub + 1) * narrow]

    def send(ring, sub, step):
        return pltpu.make_async_remote_copy(
            src_ref=acc.at[ring, sub, step], dst_ref=acc.at[ring, sub, step + 1], send_sem=send_sem.at[ring, sub],
            recv_sem=recv_sem.at[ring, sub, step], device_id={"tp": nexts[ring]}, device_id_type=MESH_ID)

    compute(0, 0, True)
    for sub in range(SUBS):
        down(sub)
        for ring in range(RINGS):
            acc[ring, sub, 0] = mine(ring, sub).astype(BF16)
            send(ring, sub, 0).start()

    @pl.loop(1, last)
    def _(step):
        compute(step, lax.rem(step, 2), True)
        for sub in range(SUBS):
            down(sub)
            for ring in range(RINGS):
                send(ring, sub, step - 1).wait_recv()
                acc[ring, sub, step] = (acc[ring, sub, step].astype(F32) + mine(ring, sub)).astype(BF16)
                send(ring, sub, step).start()

    compute(last, last % 2, False)
    for sub in range(SUBS):
        down(sub)
        for ring in range(RINGS):
            send(ring, sub, last - 1).wait_recv()

    chunk = 16
    per = share // chunk

    @pl.loop(0, rows // chunk)
    def _(i):
        rs = pl.ds(pl.multiple_of(i * chunk, chunk), chunk)
        sub = pl.ds(pl.multiple_of(lax.rem(i, per) * chunk, chunk), chunk)
        total = jnp.concatenate([acc[lax.div(i, per), half, last, sub] for half in range(SUBS)], axis=1).astype(F32) + part[rs]
        new = (res_ref[rs].astype(F32) + total.astype(BF16).astype(F32)).astype(BF16)
        x_ref[rs] = new
        if n_ref is not None:
            n_ref[rs] = layer_norm(new, gain_ref[...], bias_ref[...])

    for ring in range(RINGS):
        for sub in range(SUBS):
            done = acc.at[ring, sub, pl.ds(0, last)]
            pltpu.make_async_copy(done, done, send_sem.at[ring, sub]).wait()


def reduce_layer(torus, layer, from_normed, last_layer, source, ctxs, w_outs, w_downs, w_ups, residual, gain, bias):
    rows, d_model = residual.shape
    heads, cols = ctxs[0].shape[2], w_downs[0].shape[1]
    depth = CORES * (heads + cols)
    share = rows // RINGS
    anys = [pl.BlockSpec(memory_space=pl.ANY)] * 9
    vmem = pl.BlockSpec(memory_space=pltpu.VMEM)
    n_out = 1 if last_layer else 2
    return pl.pallas_call(
        functools.partial(reduce_kernel, torus, layer, from_normed, last_layer),
        name=f"reduce_layer_{layer}",
        out_shape=[jax.ShapeDtypeStruct((rows, d_model), BF16)] * n_out,
        in_specs=[*anys, vmem, vmem, vmem],
        out_specs=[vmem] * n_out,
        scratch_shapes=[
            pltpu.VMEM((torus.chips, rows, CORES * heads), BF16),
            pltpu.VMEM((depth, d_model), BF16),
            pltpu.VMEM((d_model, CORES * cols) if from_normed else (16, 128), BF16),
            pltpu.VMEM((2, rows, source.shape[2]), BF16),
            pltpu.VMEM((rows, depth), BF16),
            pltpu.VMEM((rows, d_model), F32),
            pltpu.VMEM((RINGS, SUBS, torus.chips, share, d_model // SUBS), BF16),
            pltpu.SemaphoreType.DMA((8,)),
            pltpu.SemaphoreType.DMA((2, RINGS)),
            pltpu.SemaphoreType.DMA((RINGS, SUBS)),
            pltpu.SemaphoreType.DMA((RINGS, SUBS, torus.chips - 1)),
        ],
        compiler_params=pltpu.CompilerParams(collective_id=3 + layer, has_side_effects=True, vmem_limit_bytes=VMEM_LIMIT),
    )(source, *ctxs, *w_outs, *w_downs, *w_ups, residual, gain.reshape(1, -1), bias.reshape(1, -1))


def project_kernel(torus, layer, n_ref, wq0, wq1, wu0, wu1, qkv_ref, up_ref, w_buf, got, stage, load_sem, send_sem, recv_sem):
    core, x, y = torus.me()
    pos = [torus.position(ring, x, y) for ring in range(RINGS)]
    rows = n_ref.shape[0]
    share = rows // RINGS
    last = torus.chips - 1
    copies = []
    start = 0
    for i, w_src in enumerate((wq0, wq1, wu0, wu1)):
        width = w_src.shape[2]
        copies.append(pltpu.make_async_copy(w_src.at[layer], w_buf.at[:, pl.ds(start, width)], load_sem.at[i]))
        start += width
    own_chip = y * torus.side + x
    own = pltpu.make_async_copy(n_ref, got.at[own_chip], load_sem.at[4])
    own.start()
    for copy in copies:
        copy.start()
    nexts = enter(torus, core, pos)
    own.wait()

    def block(ring, step):
        return torus.chip_at(ring, pos[ring] - torus.sign(ring) * step)

    def piece(ring, step):
        return got.at[block(ring, step), pl.ds(ring * share, share)]

    def send(ring, step):
        return pltpu.make_async_remote_copy(
            src_ref=piece(ring, step), dst_ref=piece(ring, step), send_sem=send_sem.at[ring],
            recv_sem=recv_sem.at[ring, step], device_id={"tp": nexts[ring]}, device_id_type=MESH_ID)

    def arrived(ring, step):
        return pltpu.make_async_remote_copy(
            src_ref=piece(ring, step + 1), dst_ref=piece(ring, step + 1), send_sem=send_sem.at[ring],
            recv_sem=recv_sem.at[ring, step], device_id={"tp": nexts[ring]}, device_id_type=MESH_ID)

    tile = 256

    def compute(step):
        for ring in range(RINGS):
            stage[pl.ds(ring * share, share)] = got[block(ring, step), pl.ds(ring * share, share)]

        @pl.loop(0, qkv_ref.shape[2] // tile)
        def _(j):
            cs = pl.ds(pl.multiple_of(j * tile, tile), tile)
            res = jnp.dot(stage[...], w_buf[:, cs], preferred_element_type=F32)
            for ring in range(RINGS):
                rs = slice(ring * share, (ring + 1) * share)
                qkv_ref[block(ring, step), rs, cs] = res[rs]

        @pl.loop(0, up_ref.shape[2] // tile)
        def _(j):
            off = pl.multiple_of(j * tile, tile)
            res = jnp.dot(stage[...], w_buf[:, pl.ds(pl.multiple_of(qkv_ref.shape[2] + off, tile), tile)], preferred_element_type=F32)
            act = gelu(res).astype(BF16)
            for ring in range(RINGS):
                rs = slice(ring * share, (ring + 1) * share)
                up_ref[block(ring, step), rs, pl.ds(off, tile)] = act[rs]

    for ring in range(RINGS):
        send(ring, 0).start()
    for copy in copies:
        copy.wait()
    compute(0)

    @pl.loop(1, last)
    def _(step):
        for ring in range(RINGS):
            arrived(ring, step - 1).wait_recv()
            send(ring, step).start()
        compute(step)

    for ring in range(RINGS):
        arrived(ring, last - 1).wait_recv()
    compute(last)
    for ring in range(RINGS):
        done = got.at[pl.ds(0, last), pl.ds(ring * share, share)]
        pltpu.make_async_copy(done, done, send_sem.at[ring]).wait()


def gather_project(torus, layer, normed, w_qkvs, w_ups):
    rows, d_model = normed.shape
    n_qkv, n_up = CORES * w_qkvs[0].shape[2], CORES * w_ups[0].shape[2]
    width = n_qkv + n_up
    anys = [pl.BlockSpec(memory_space=pl.ANY)] * 5
    return pl.pallas_call(
        functools.partial(project_kernel, torus, layer),
        name="gather_project",
        out_shape=[jax.ShapeDtypeStruct((torus.chips, rows, n_qkv), F32), jax.ShapeDtypeStruct((torus.chips, rows, n_up), BF16)],
        in_specs=anys,
        out_specs=[pl.BlockSpec(memory_space=pltpu.VMEM)] * 2,
        scratch_shapes=[
            pltpu.VMEM((d_model, width), BF16),
            pltpu.VMEM((torus.chips, rows, d_model), BF16),
            pltpu.VMEM((rows, d_model), BF16),
            pltpu.SemaphoreType.DMA((5,)),
            pltpu.SemaphoreType.DMA((RINGS,)),
            pltpu.SemaphoreType.DMA((RINGS, torus.chips - 1)),
        ],
        compiler_params=pltpu.CompilerParams(collective_id=1, has_side_effects=True, vmem_limit_bytes=VMEM_LIMIT),
    )(normed, *w_qkvs, *w_ups)


def gather_kernel(torus, y_ref, out_ref, got, load_sem, send_sem, recv_sem, pair_sem, store_sem):
    core, x, y = torus.me()
    pos = [torus.position(ring, x, y) for ring in range(RINGS)]
    rows = y_ref.shape[0]
    share = rows // RINGS
    last = torus.chips - 1
    own_chip = y * torus.side + x
    own = pltpu.make_async_copy(y_ref, got.at[own_chip], load_sem.at[0])
    own.start()
    partner = own_chip * CORES + (CORES - 1 - core)
    nexts = enter(torus, core, pos, (partner,))
    own.wait()

    def block(ring, step):
        return torus.chip_at(ring, pos[ring] - torus.sign(ring) * step)

    thin = share // SUBS

    def piece(ring, sub, step):
        return got.at[block(ring, step), pl.ds(ring * share + sub * thin, thin)]

    def send(ring, sub, step):
        return pltpu.make_async_remote_copy(
            src_ref=piece(ring, sub, step), dst_ref=piece(ring, sub, step), send_sem=send_sem.at[ring, sub],
            recv_sem=recv_sem.at[ring, sub, step], device_id={"tp": nexts[ring]}, device_id_type=MESH_ID)

    def arrived(ring, sub, step):
        return pltpu.make_async_remote_copy(
            src_ref=piece(ring, sub, step + 1), dst_ref=piece(ring, sub, step + 1), send_sem=send_sem.at[ring, sub],
            recv_sem=recv_sem.at[ring, sub, step], device_id={"tp": nexts[ring]}, device_id_type=MESH_ID)

    def spread(ring, step):
        src = got.at[block(ring, step), pl.ds(ring * share, share)]
        dst = out_ref.at[core * torus.chips + block(ring, step), pl.ds(ring * share, share)]
        pltpu.make_async_remote_copy(
            src_ref=src, dst_ref=dst, send_sem=pair_sem.at[0], recv_sem=pair_sem.at[1],
            device_id={"tp": partner}, device_id_type=MESH_ID).start()
        pltpu.make_async_copy(src, dst, store_sem.at[0]).start()

    for sub in range(SUBS):
        for ring in range(RINGS):
            send(ring, sub, 0).start()
    for ring in range(RINGS):
        spread(ring, 0)

    @pl.loop(1, last)
    def _(step):
        for sub in range(SUBS):
            for ring in range(RINGS):
                arrived(ring, sub, step - 1).wait_recv()
                send(ring, sub, step).start()
        for ring in range(RINGS):
            spread(ring, step)

    for ring in range(RINGS):
        for sub in range(SUBS):
            arrived(ring, sub, last - 1).wait_recv()
        spread(ring, last)
    for ring in range(RINGS):
        for sub in range(SUBS):
            done = got.at[pl.ds(0, last), pl.ds(ring * share + sub * thin, thin)]
            pltpu.make_async_copy(done, done, send_sem.at[ring, sub]).wait()
    pltpu.make_async_copy(got, got, pair_sem.at[0]).wait()
    pltpu.make_async_copy(got, got, store_sem.at[0]).wait()
    pltpu.make_async_copy(got, got, pair_sem.at[1]).wait()


def gather_all(torus, y_own):
    rows, d_model = y_own.shape
    return pl.pallas_call(
        functools.partial(gather_kernel, torus),
        name="gather_all",
        out_shape=jax.ShapeDtypeStruct((CORES * torus.chips, rows, d_model), BF16),
        in_specs=[pl.BlockSpec(memory_space=pl.ANY)],
        out_specs=pl.BlockSpec(memory_space=pl.ANY),
        scratch_shapes=[
            pltpu.VMEM((torus.chips, rows, d_model), BF16),
            pltpu.SemaphoreType.DMA((1,)),
            pltpu.SemaphoreType.DMA((RINGS, SUBS)),
            pltpu.SemaphoreType.DMA((RINGS, SUBS, torus.chips - 1)),
            pltpu.SemaphoreType.DMA((2,)),
            pltpu.SemaphoreType.DMA((1,)),
        ],
        compiler_params=pltpu.CompilerParams(collective_id=2, has_side_effects=True, vmem_limit_bytes=VMEM_LIMIT),
    )(y_own)


def solution(mesh):
    n_tp = mesh.shape["tp"]
    torus = Torus(math.isqrt(n_tp // CORES))
    swap = [(i, i ^ 1) for i in range(n_tp)]

    def shard_body(act_in, ln_gain, ln_bias, w_qkv, w_out, w_up, w_down):
        layers = ln_gain.shape[0]
        head_dim = w_out.shape[1]
        idx = lax.axis_index("tp")
        core, chip = lax.rem(idx, CORES), lax.div(idx, CORES)
        w_qkv = w_qkv[:, :, 0]
        w_qkvs, w_ups, w_outs, w_downs = [(w, lax.ppermute(w, "tp", swap)) for w in (w_qkv, w_up, w_out, w_down)]

        half = lax.dynamic_slice_in_dim(act_in, core * torus.chips, torus.chips, 0)
        own = lax.dynamic_index_in_dim(half, chip, 0, keepdims=False)
        normed = layer_norm(half, ln_gain[0], ln_bias[0])
        for layer in range(layers):
            if layer == 0:
                source = normed
                qkvs = [jnp.einsum("bsd,dc->bsc", normed, w[layer], preferred_element_type=F32) for w in w_qkvs]
            else:
                qkv, source = gather_project(torus, layer, normed, w_qkvs, w_ups)
                n_qkv = w_qkv.shape[2]
                qkvs = [qkv[..., i * n_qkv:(i + 1) * n_qkv] for i in range(CORES)]
            ctxs = [attend(qkv, head_dim) for qkv in qkvs]
            nxt = (layer + 1) % layers
            outs = reduce_layer(torus, layer, layer == 0, layer == layers - 1, source, ctxs, w_outs, w_downs, w_ups, own, ln_gain[nxt], ln_bias[nxt])
            own, normed = outs[0], outs[-1]
        return gather_all(torus, own)

    return jax.shard_map(shard_body, mesh=mesh, in_specs=(P("dp", None, None), P(None, None), P(None, None), P(None, None, "tp", None), P(None, "tp", None), P(None, None, "tp"), P(None, "tp", None)), out_specs=P("dp", None, None), check_vma=False)
```
